32 devices in a mesh: dp: 4 (over x, core), section: 2 (over y), mp: 4 (over z).
Axes of the slice: x: 2, y: 2, z: 4, core: 2. Of those that a mesh axis runs over, the one named last changes fastest.
Arguments:
- micro_inputs: bfloat16 [8, 64, 4096], P(('dp', 'section'), None, 'mp'), parts along dimension 0, may hold values from -6 to 6
- qkv_weight: bfloat16 [2, 4096, 3, 2048], P('section', None, None, 'mp'), may hold values from -0.09375 to 0.09375
- out_weight: bfloat16 [2, 2048, 4096], P('section', None, 'mp'), may hold values from -0.125 to 0.125
- norm_gain: bfloat16 [2, 4096], P('section'), may hold values from 0.099609375 to 1.8984375
- position_bias: float32 [32, 32], P('mp'), may hold values from -3 to 280
Outputs:
- encoded: bfloat16 [8, 64, 4096], P(('dp', 'section'), None, 'mp'), parts along dimension 0
The draws below stay inside these ranges and needn't reach their ends.
There are 4 independent parts, one for each index of `dp`. The reference program is written for one: setup_inputs(seed, part) draws one part's arguments, and reference() takes and returns one part's arrays. A program takes and returns all parts, laid end to end along the dimension named above; an argument that names none is the same for every part. Nothing has to cross between parts.
All inputs are finite; a program needn't handle non-finite values.
Results may differ from the reference program's by a relative error of at most 0.025.
Values may be sent and summed in bfloat16 or wider, within the bound.
A program may use at most 128 MiB of HBM per device.

```python
import math
import jax
import jax.numpy as jnp
import numpy as np
from jax import lax

D = 4096
HS = 64
HEADS = 32
BUCKETS = 32
REACH = 128
LENGTH = 64
LAYERS = 2
MICROS = 2


def draw_position_bias(key, part):
    ordinary = jnp.clip(jax.random.normal(key, (HEADS, BUCKETS), jnp.float32), -3.0, 3.0)
    return ordinary


def shard_levels(rng, dims, shards, smallest, largest):
    def one(position, parts):
        steps = jax.random.uniform(jax.random.fold_in(jax.random.fold_in(rng, 6), position), (parts,), jnp.float32, smallest / len(shards), largest / len(shards))
        return jnp.repeat(jnp.exp(steps), dims[position] // parts).reshape((-1,) + (1,) * (len(dims) - position - 1))

    level = one(*shards[0])
    for cut in shards[1:]:
        level = level * one(*cut)
    return level


def centred(rng, shape, scale, most, split=(), kind=jnp.bfloat16):
    values = scale * jax.random.normal(rng, shape, jnp.float32)
    if split:
        values = values * shard_levels(rng, shape, split, -0.22, 0.18)
    return jnp.clip(values, -most, most).astype(kind)


def setup_inputs(seed: int = 0, part: int = 0) -> dict:
    seeds = jax.random.split(jax.random.key(seed), 6)
    own_keys = jax.random.split(jax.random.fold_in(seeds[5], part), 6)
    micro_inputs = centred(own_keys[0], (MICROS, LENGTH, D), 1.0, 6.0, ((0, 2), (2, 4)))
    qkv_weight = centred(seeds[1], (LAYERS, D, 3, HEADS * HS), D ** -0.5, 0.09375, ((0, 2), (3, 4)))
    out_weight = centred(seeds[2], (LAYERS, HEADS * HS, D), (HEADS * HS) ** -0.5, 0.125, ((0, 2), (2, 4)))
    norm_gain = jnp.clip(1.0 + 0.18 * jax.random.normal(seeds[3], (LAYERS, D), jnp.float32), 0.099609375, 1.8984375).astype(jnp.bfloat16)
    position_bias = draw_position_bias(jax.random.fold_in(seeds[5], 71), part)
    return {"micro_inputs": micro_inputs, "qkv_weight": qkv_weight, "out_weight": out_weight, "norm_gain": norm_gain, "position_bias": position_bias}


NORM_EPSILON = 0.1

def bucket_table(length, bucket_count, reach_limit):
    offset = np.arange(length)[None, :] - np.arange(length)[:, None]
    half_count = bucket_count // 2
    upper_side = (offset > 0).astype(np.int32) * half_count
    distance = np.abs(offset)
    exact_count = half_count // 2
    scaled = np.log(np.maximum(distance, 1) / exact_count) / np.log(reach_limit / exact_count) * (half_count - exact_count)
    far_bucket = np.minimum(exact_count + scaled.astype(np.int32), half_count - 1)
    return (upper_side + np.where(distance < exact_count, distance, far_bucket)).astype(np.int32)

def reference(micro_inputs, qkv_weight, out_weight, norm_gain, position_bias):
    bucket_grid = jnp.asarray(bucket_table(LENGTH, BUCKETS, REACH)).astype(jnp.int32)
    score_bias = position_bias[:, bucket_grid].astype(jnp.float32)
    score_scale = 1.0 / math.sqrt(HS)

    def layer_step(hidden, layer_index):
        stream = hidden.astype(jnp.float32)
        mean_square = lax.optimization_barrier(jnp.mean(stream * stream, axis=1, keepdims=True))
        row_scale = lax.rsqrt(mean_square + NORM_EPSILON)
        gained = (stream * norm_gain[layer_index].astype(jnp.float32)).astype(jnp.bfloat16)
        weight_grid = qkv_weight[layer_index].reshape(D, 3 * HEADS * HS)
        project = jnp.dot(gained, weight_grid, preferred_element_type=jnp.float32) * row_scale
        rounded = lax.optimization_barrier(project.astype(jnp.bfloat16))
        project = rounded.astype(jnp.float32).reshape(LENGTH, 3, HEADS, HS)
        queries = project[:, 0]
        key_heads = project[:, 1]
        values = project[:, 2]
        scores = jnp.einsum('ihd,jhd->hij', queries, key_heads, precision=lax.Precision.HIGHEST) * score_scale + score_bias
        row_max = lax.optimization_barrier(jnp.max(scores, axis=2, keepdims=True))
        weights = jnp.exp(scores - row_max)
        attn_probs = lax.optimization_barrier((weights / lax.optimization_barrier(jnp.sum(weights, axis=2, keepdims=True))).astype(jnp.bfloat16))
        head_mix = jnp.einsum('hij,jhd->ihd', attn_probs.astype(jnp.float32), values, precision=lax.Precision.HIGHEST)
        head_mix = head_mix.astype(jnp.bfloat16).reshape(LENGTH, HEADS * HS)
        update = jnp.dot(head_mix, out_weight[layer_index], preferred_element_type=jnp.float32)
        return ((stream + update).astype(jnp.bfloat16), None)

    def run_micro(micro_rows):
        finished, unused = lax.scan(layer_step, micro_rows, jnp.arange(LAYERS, dtype=jnp.int32))
        return finished
    return lax.map(run_micro, micro_inputs)
```

```python
import functools
import math

import jax
import jax.numpy as jnp
import numpy as np
from jax import lax
from jax.experimental import pallas as pl
from jax.experimental.pallas import tpu as pltpu
from jax.sharding import PartitionSpec as P

REACH = 128
NORM_EPSILON = 0.1
MESH = pl.DeviceIdType.MESH


def bucket_table(length, bucket_count, reach_limit):
    offset = np.arange(length)[None, :] - np.arange(length)[:, None]
    half_count = bucket_count // 2
    upper_side = (offset > 0).astype(np.int32) * half_count
    distance = np.abs(offset)
    exact_count = half_count // 2
    scaled = (
        np.log(np.maximum(distance, 1) / exact_count)
        / np.log(reach_limit / exact_count)
        * (half_count - exact_count)
    )
    far_bucket = np.minimum(exact_count + scaled.astype(np.int32), half_count - 1)
    return (upper_side + np.where(distance < exact_count, distance, far_bucket)).astype(np.int32)


def relay_chunks(rows):
    units = rows // 16
    here = max(1, (3 * units) // 8)
    there = units - here
    first = (there + 1) // 2
    cuts = [(0, first * 16), (first * 16, (there - first) * 16)]
    return [c for c in cuts if c[1]], (there * 16, here * 16)


def kernel(
    sizes,
    x_ref, gain_ref, bucket_ref, pbias_ref, wq_hbm, wo_hbm,
    o_ref,
    pre, xg, hg, spread, ho, fin, wq, wo, acc, acc2, sq, qkv, bias,
    wq_sem, wo_sem,
    pre_recv, pre_send, pre_up, in_recv,
    hop_send, hop_recv, hop_line,
    spread_recv, spread_send, spread_up, late_recv,
    mix_recv, mix_send,
    fin_send, fin_recv,
):
    S, M, L, H, hs = sizes
    Dl = x_ref.shape[1]
    Wl = H * hs
    R = S * L
    D = M * Dl
    s = lax.axis_index("section")
    m = lax.axis_index("mp")
    hops, (late_at, late_rows) = relay_chunks(R)
    late = pl.ds(late_at, late_rows)

    def to(src, dst, send, recv, sec, col):
        return pltpu.make_async_remote_copy(
            src_ref=src, dst_ref=dst, send_sem=send, recv_sem=recv,
            device_id={"section": sec, "mp": col}, device_id_type=MESH,
        )

    def along(j, src, dst, send, recv, act):
        @pl.when((j <= m) & (m < M - 1))
        def _():
            act(to(src, dst, send.at[0, j], recv, s, m + 1))

        @pl.when((j >= m) & (m > 0))
        def _():
            act(to(src, dst, send.at[1, j], recv, s, m - 1))

    def start(c):
        c.start()

    def sent(c):
        c.wait_send()

    def got(dst, recv):
        to(dst, dst, fin_send.at[0], recv, s, lax.rem(m + 1, M)).wait_recv()

    near = jnp.minimum(m, M - 1 - m)
    longer = jnp.where(m > M - 1 - m, -1, 1)

    def nth(p):
        k = (p + 1) // 2
        both = jnp.where(p % 2 == 1, -k, k)
        return m + jnp.where(p <= 2 * near, both, longer * (p - near))

    def wq_copy(j):
        rows = pl.ds(pl.multiple_of(j * Dl, Dl), Dl)
        return pltpu.make_async_copy(wq_hbm.at[:, rows, :], wq.at[:, rows, :], wq_sem.at[j])

    def wo_copy():
        return pltpu.make_async_copy(wo_hbm, wo, wo_sem)

    for p in range(M):
        wq_copy(nth(p)).start()
    wo_copy().start()

    barrier = pltpu.get_barrier_semaphore()

    @pl.when(m > 0)
    def _():
        pl.semaphore_signal(barrier, inc=1, device_id={"section": s, "mp": m - 1}, device_id_type=MESH)

    @pl.when(m < M - 1)
    def _():
        pl.semaphore_signal(barrier, inc=1, device_id={"section": s, "mp": m + 1}, device_id_type=MESH)

    for k in range(1, S):
        pl.semaphore_signal(
            barrier, inc=1, device_id={"section": lax.rem(s + k, S), "mp": m}, device_id_type=MESH
        )
    pl.semaphore_wait(
        barrier, S - 1 + jnp.where(m > 0, 1, 0) + jnp.where(m < M - 1, 1, 0)
    )

    def up_rows(j):
        return xg.at[j, pl.ds(pl.multiple_of(s * L, L), L), :]

    def first_act(act):
        along(m, x_ref, pre.at[m], pre_send, pre_recv.at[m], act)

        @pl.when(s > 0)
        def _():
            act(to(x_ref, up_rows(m), pre_up.at[m], in_recv.at[s, m], 0, m))

    def pre_act(j, act):
        along(j, pre.at[j], pre.at[j], pre_send, pre_recv.at[j], act)

        @pl.when(s > 0)
        def _():
            act(to(pre.at[j], up_rows(j), pre_up.at[j], in_recv.at[s, j], 0, m))

    first_act(start)

    @pl.when(s == 0)
    def _():
        xg[m, 0:L, :] = x_ref[...]

    for h in range(H):
        total = jnp.zeros(bucket_ref.shape, jnp.float32)
        for b in range(pbias_ref.shape[1]):
            total = jnp.where(bucket_ref[...] == b, pbias_ref[h, b], total)
        bias[h] = total
    acc[...] = jnp.zeros_like(acc)
    acc2[...] = jnp.zeros_like(acc2)
    sq[...] = jnp.zeros_like(sq)

    def pre_step(p, carry):
        j = nth(p)
        got(pre.at[j], pre_recv.at[j])
        pre_act(j, start)

        @pl.when(s == 0)
        def _():
            xg[j, 0:L, :] = pre[j]

        return carry

    lax.fori_loop(1, M, pre_step, 0)

    def hop_act(c, j, act):
        at, rows = hops[c]
        block = xg.at[j, pl.ds(at, rows), :]
        along(j, block, block, hop_line.at[c], hop_recv.at[c, j], act)

    def qkv_step(p, carry):
        j = nth(p)

        @pl.when(s == 0)
        def _():
            for o in range(1, S):
                got(xg.at[j, pl.ds(o * L, L), :], in_recv.at[o, j])

        @pl.when(s > 0)
        def _():
            for c, (at, rows) in enumerate(hops):
                got(xg.at[j, pl.ds(at, rows), :], hop_recv.at[c, j])
                hop_act(c, j, start)
            got(xg.at[j, late, :], late_recv.at[j])

        wq_copy(j).wait()
        block = xg[j].astype(jnp.float32)
        squares = block * block
        part = squares[:, 0:128]
        for k in range(1, Dl // 128):
            part = part + squares[:, k * 128 : (k + 1) * 128]
        sq[...] += part
        gained = (block * gain_ref[j]).astype(jnp.bfloat16)
        rows = pl.ds(pl.multiple_of(j * Dl, Dl), Dl)
        for t in range(3):
            cols = pl.ds(t * Wl, Wl)
            acc[:, cols] += jnp.dot(gained, wq[t, rows, :], preferred_element_type=jnp.float32)
        return carry

    lax.fori_loop(0, M, qkv_step, 0)
    row_scale = lax.rsqrt(jnp.sum(sq[...], axis=1, keepdims=True) / D + NORM_EPSILON)
    qkv[...] = (acc[...] * row_scale).astype(jnp.bfloat16)

    mix_rows = L * ((S + 1) // 2)
    mixes = [(at, min(mix_rows, R - at)) for at in range(0, R, mix_rows)]

    def mix_act(c, j, act):
        at, rows = mixes[c]
        block = hg.at[j, pl.ds(at, rows), :]
        along(j, block, block, mix_send.at[c], mix_recv.at[c, j], act)

    scale = 1.0 / math.sqrt(hs)

    def attend(at):
        rows = pl.ds(at, L)
        outs = []
        for h in range(H):
            q = qkv[rows, h * hs : (h + 1) * hs]
            k = qkv[rows, Wl + h * hs : Wl + (h + 1) * hs]
            v = qkv[rows, 2 * Wl + h * hs : 2 * Wl + (h + 1) * hs]
            scores = lax.dot_general(
                q, k, (((1,), (1,)), ((), ())), preferred_element_type=jnp.float32
            ) * scale + bias[h]
            weights = jnp.exp(scores - jnp.max(scores, axis=1, keepdims=True))
            probs = (weights / jnp.sum(weights, axis=1, keepdims=True)).astype(jnp.bfloat16)
            outs.append(jnp.dot(probs, v, preferred_element_type=jnp.float32).astype(jnp.bfloat16))
        hg[m, rows, :] = jnp.concatenate(outs, axis=1)

    for c, (at, rows) in enumerate(mixes):
        if rows == L:
            attend(at)
        else:
            def attend_step(i, carry):
                attend(pl.multiple_of(at + i * L, L))
                return carry

            lax.fori_loop(0, rows // L, attend_step, 0)
        mix_act(c, m, start)

    wo_copy().wait()

    def project(j):
        rows = pl.ds(pl.multiple_of(j * Wl, Wl), Wl)
        acc2[...] += jnp.dot(hg[j], wo[rows, :], preferred_element_type=jnp.float32)

    project(m)

    def mix_step(p, carry):
        j = nth(p)
        for c, (at, rows) in enumerate(mixes):
            got(hg.at[j, pl.ds(at, rows), :], mix_recv.at[c, j])
            mix_act(c, j, start)
        project(j)
        return carry

    lax.fori_loop(1, M, mix_step, 0)
    ho[...] = (xg[m].astype(jnp.float32) + acc2[...]).astype(jnp.bfloat16)

    own_late = ho.at[late, :]

    def hop_out(act):
        for c, (at, rows) in enumerate(hops):
            act(to(ho.at[pl.ds(at, rows), :], xg.at[m, pl.ds(at, rows), :],
                   hop_send.at[c], hop_recv.at[c, m], s + 1, m))

    def late_out(j, src, act):
        along(j, src, spread.at[j], spread_send, spread_recv.at[j], act)
        act(to(src, xg.at[j, late, :], spread_up.at[j], late_recv.at[j], s + 1, m))

    def home(act):
        for o in range(S - 1):
            act(to(ho.at[pl.ds(o * L, L), :], fin, fin_send.at[o], fin_recv, o, m))

    @pl.when(s < S - 1)
    def _():
        hop_out(start)
        late_out(m, own_late, start)

        def late_step(p, carry):
            j = nth(p)
            got(spread.at[j], spread_recv.at[j])
            late_out(j, spread.at[j], start)
            return carry

        lax.fori_loop(1, M, late_step, 0)

    @pl.when(s == S - 1)
    def _():
        home(start)
        o_ref[...] = ho[(S - 1) * L :, :]

    first_act(sent)
    for c in range(len(mixes)):
        mix_act(c, m, sent)

    @pl.when(s > 0)
    def _():
        for c in range(len(hops)):
            hop_act(c, m, sent)

    @pl.when(s < S - 1)
    def _():
        hop_out(sent)
        late_out(m, own_late, sent)

    def drain_step(p, carry):
        j = nth(p)
        pre_act(j, sent)
        for c in range(len(mixes)):
            mix_act(c, j, sent)

        @pl.when(s > 0)
        def _():
            for c in range(len(hops)):
                hop_act(c, j, sent)

        @pl.when(s < S - 1)
        def _():
            late_out(j, spread.at[j], sent)

        return carry

    lax.fori_loop(1, M, drain_step, 0)

    @pl.when(s == S - 1)
    def _():
        home(sent)

    @pl.when(s < S - 1)
    def _():
        got(fin, fin_recv)
        o_ref[...] = fin[...]


def solution(mesh):
    S, M = mesh.shape["section"], mesh.shape["mp"]

    def shards(micro_inputs, qkv_weight, out_weight, norm_gain, position_bias):
        L, Dl = micro_inputs.shape[1:]
        D = qkv_weight.shape[1]
        Wl = qkv_weight.shape[3]
        H = position_bias.shape[0]
        R = S * L
        hops, (_, late_rows) = relay_chunks(R)
        mixes = -(-R // (L * ((S + 1) // 2)))
        buckets = jnp.asarray(bucket_table(L, position_bias.shape[1], REACH))
        gain = norm_gain.reshape(M, 1, Dl).astype(jnp.float32)
        wq = jnp.transpose(qkv_weight[0], (1, 0, 2))
        bf16, f32 = jnp.bfloat16, jnp.float32
        dma = pltpu.SemaphoreType.DMA
        vmem = pl.BlockSpec(memory_space=pltpu.VMEM)
        out = pl.pallas_call(
            functools.partial(kernel, (S, M, L, H, Wl // H)),
            out_shape=jax.ShapeDtypeStruct((L, Dl), bf16),
            in_specs=[
                vmem, vmem, vmem, pl.BlockSpec(memory_space=pltpu.SMEM),
                pl.BlockSpec(memory_space=pl.ANY), pl.BlockSpec(memory_space=pl.ANY),
            ],
            out_specs=vmem,
            scratch_shapes=[
                pltpu.VMEM((M, L, Dl), bf16),
                pltpu.VMEM((M, R, Dl), bf16),
                pltpu.VMEM((M, R, Wl), bf16),
                pltpu.VMEM((M, late_rows, Dl), bf16),
                pltpu.VMEM((R, Dl), bf16),
                pltpu.VMEM((L, Dl), bf16),
                pltpu.VMEM((3, D, Wl), bf16),
                pltpu.VMEM((M * Wl, Dl), bf16),
                pltpu.VMEM((R, 3 * Wl), f32),
                pltpu.VMEM((R, Dl), f32),
                pltpu.VMEM((R, 128), f32),
                pltpu.VMEM((R, 3 * Wl), bf16),
                pltpu.VMEM((H, L, L), f32),
                dma((M,)), dma,
                dma((M,)), dma((2, M)), dma((M,)), dma((S, M)),
                dma((len(hops),)), dma((len(hops), M)), dma((len(hops), 2, M)),
                dma((M,)), dma((2, M)), dma((M,)), dma((M,)),
                dma((mixes, M)), dma((mixes, 2, M)),
                dma((S,)), dma,
            ],
            compiler_params=pltpu.CompilerParams(
                collective_id=0, has_side_effects=True, vmem_limit_bytes=60 * 1024 * 1024
            ),
        )(micro_inputs[0], gain, buckets, position_bias, wq, out_weight[0])
        return out[None]

    in_specs = (
        P(("dp", "section"), None, "mp"),
        P("section", None, None, "mp"),
        P("section", None, "mp"),
        P("section", None),
        P("mp", None),
    )
    out_specs = P(("dp", "section"), None, "mp")
    return jax.shard_map(shards, mesh=mesh, in_specs=in_specs, out_specs=out_specs, check_vma=False)
```

```python
import functools
import math

import jax
import jax.numpy as jnp
import numpy as np
from jax import lax
from jax.experimental import pallas as pl
from jax.experimental.pallas import tpu as pltpu
from jax.sharding import PartitionSpec as P

REACH = 128
NORM_EPSILON = 0.1
MESH = pl.DeviceIdType.MESH


def bucket_table(length, bucket_count, reach_limit):
    offset = np.arange(length)[None, :] - np.arange(length)[:, None]
    half_count = bucket_count // 2
    upper_side = (offset > 0).astype(np.int32) * half_count
    distance = np.abs(offset)
    exact_count = half_count // 2
    scaled = (
        np.log(np.maximum(distance, 1) / exact_count)
        / np.log(reach_limit / exact_count)
        * (half_count - exact_count)
    )
    far_bucket = np.minimum(exact_count + scaled.astype(np.int32), half_count - 1)
    return (upper_side + np.where(distance < exact_count, distance, far_bucket)).astype(np.int32)


def relay_chunks(micro, micros, length):
    here = length // 2 // 16 * 16 if micro == micros - 1 else 0
    there = length - here
    half = max(16, there // 2 // 16 * 16)
    return [(at, min(half, there - at)) for at in range(0, there, half)], (there, here)


def head_group(heads, head_size):
    return max(g for g in range(1, heads + 1) if heads % g == 0 and g * head_size <= 256)


def kernel(
    sizes,
    x_ref, gain_ref, bucket_ref, pbias_ref, wq_hbm, wo_hbm,
    o_ref,
    pre, xg, hg, spread, ho, fin, wq, wo, acc, sq, qkv, bias, head_mask,
    wq_sem, wo_sem,
    pre_recv, pre_send, pre_up, in_recv,
    hop_send, hop_recv, hop_line,
    spread_recv, spread_send, spread_up, late_recv,
    mix_recv, mix_send,
    fin_send, fin_recv,
):
    S, M, L, H, hs = sizes
    Dl = x_ref.shape[1]
    Wl = H * hs
    G = head_group(H, hs)
    Wg = G * hs
    D = M * Dl
    s = lax.axis_index("section")
    m = lax.axis_index("mp")
    plans = [relay_chunks(i, S, L) for i in range(S)]

    def to(src, dst, send, recv, sec, col):
        return pltpu.make_async_remote_copy(
            src_ref=src, dst_ref=dst, send_sem=send, recv_sem=recv,
            device_id={"section": sec, "mp": col}, device_id_type=MESH,
        )

    def along(j, src, dst, send, recv, act):
        @pl.when((j <= m) & (m < M - 1))
        def _():
            act(to(src, dst, send.at[0, j], recv, s, m + 1))

        @pl.when((j >= m) & (m > 0))
        def _():
            act(to(src, dst, send.at[1, j], recv, s, m - 1))

    def start(c):
        c.start()

    def sent(c):
        c.wait_send()

    def got(dst, recv):
        to(dst, dst, fin_send.at[0], recv, s, lax.rem(m + 1, M)).wait_recv()

    near = jnp.minimum(m, M - 1 - m)
    longer = jnp.where(m > M - 1 - m, -1, 1)

    def nth(p):
        k = (p + 1) // 2
        both = jnp.where(p % 2 == 1, -k, k)
        return m + jnp.where(p <= 2 * near, both, longer * (p - near))

    def wq_copy(j):
        rows = pl.ds(pl.multiple_of(j * Dl, Dl), Dl)
        return pltpu.make_async_copy(wq_hbm.at[:, rows, :], wq.at[:, rows, :], wq_sem.at[j])

    def wo_copy():
        return pltpu.make_async_copy(wo_hbm, wo, wo_sem)

    barrier = pltpu.get_barrier_semaphore()
    for k in range(1, M):
        pl.semaphore_signal(
            barrier, inc=1, device_id={"section": s, "mp": lax.rem(m + k, M)}, device_id_type=MESH
        )
    for k in range(1, S):
        pl.semaphore_signal(
            barrier, inc=1, device_id={"section": lax.rem(s + k, S), "mp": m}, device_id_type=MESH
        )

    for p in range(M):
        wq_copy(nth(p)).start()
    wo_copy().start()
    pl.semaphore_wait(barrier, S + M - 2)

    def up_rows(j):
        return xg.at[j, pl.ds(pl.multiple_of(s * L, L), L), :]

    def first_act(act):
        along(m, x_ref, pre.at[m], pre_send, pre_recv.at[m], act)

        @pl.when(s > 0)
        def _():
            act(to(x_ref, up_rows(m), pre_up.at[m], in_recv.at[s, m], 0, m))

    def pre_act(j, act):
        along(j, pre.at[j], pre.at[j], pre_send, pre_recv.at[j], act)

        @pl.when(s > 0)
        def _():
            act(to(pre.at[j], up_rows(j), pre_up.at[j], in_recv.at[s, j], 0, m))

    first_act(start)

    for g in range(H // G):
        heads = []
        for h in range(g * G, (g + 1) * G):
            total = jnp.zeros(bucket_ref.shape, jnp.float32)
            for b in range(pbias_ref.shape[1]):
                total = jnp.where(bucket_ref[...] == b, pbias_ref[h, b], total)
            heads.append(total)
        bias[g] = jnp.concatenate(heads, axis=1)
    head_mask[...] = jnp.where(
        lax.broadcasted_iota(jnp.int32, (G * L, Wg), 0) // L
        == lax.broadcasted_iota(jnp.int32, (G * L, Wg), 1) // hs,
        1.0,
        0.0,
    ).astype(jnp.bfloat16)

    @pl.when(s > 0)
    def _():
        def pre_step(p, carry):
            j = nth(p)
            got(pre.at[j], pre_recv.at[j])
            pre_act(j, start)
            return carry

        lax.fori_loop(1, M, pre_step, 0)

    def hop_block(i, c, j):
        at, rows = plans[i][0][c]
        return xg.at[j, pl.ds(i * L + at, rows), :]

    def hop_act(i, c, j, act):
        block = hop_block(i, c, j)
        along(j, block, block, hop_line.at[i, c], hop_recv.at[i, c, j], act)

    def late_block(i, j):
        at, rows = plans[i][1]
        return xg.at[j, pl.ds(i * L + at, rows), :]

    def spread_block(i, j):
        return spread.at[i, j, pl.ds(0, plans[i][1][1]), :]

    def receive(i, j):
        @pl.when(s == 0)
        def _():
            if i:
                got(xg.at[j, pl.ds(i * L, L), :], in_recv.at[i, j])
            else:
                @pl.when(j == m)
                def _():
                    xg[m, 0:L, :] = x_ref[...]

                @pl.when(j != m)
                def _():
                    got(pre.at[j], pre_recv.at[j])
                    pre_act(j, start)
                    xg[j, 0:L, :] = pre[j]

        @pl.when(s > 0)
        def _():
            for c in range(len(plans[i][0])):
                got(hop_block(i, c, j), hop_recv.at[i, c, j])
                hop_act(i, c, j, start)
            if plans[i][1][1]:
                got(late_block(i, j), late_recv.at[i, j])

    def mix_act(i, act):
        block = hg.at[pl.ds(i * L, L), pl.ds(pl.multiple_of(m * Wl, Wl), Wl)]
        for k in range(1, M):
            col = lax.rem(m + k, M)
            act(to(block, block, mix_send.at[i, k], mix_recv.at[i, m], s, col))

    scale = 1.0 / math.sqrt(hs)
    lane_head = lax.broadcasted_iota(jnp.int32, (L, Wg), 1) // hs

    def attend(i):
        for g in range(H // G):
            q = qkv[:, g * Wg : (g + 1) * Wg]
            k = qkv[:, Wl + g * Wg : Wl + (g + 1) * Wg]
            v = qkv[:, 2 * Wl + g * Wg : 2 * Wl + (g + 1) * Wg]
            apart = jnp.concatenate([q] * G, axis=0) * head_mask[...]
            scores = lax.dot_general(
                k, apart, (((1,), (1,)), ((), ())), preferred_element_type=jnp.float32
            ) * scale + bias[g]
            weights = jnp.exp(scores - jnp.max(scores, axis=0, keepdims=True))
            probs = (weights / jnp.sum(weights, axis=0, keepdims=True)).astype(jnp.bfloat16)
            mixed = lax.dot_general(
                probs, v, (((0,), (0,)), ((), ())), preferred_element_type=jnp.float32
            )
            out = mixed[0:L]
            for h in range(1, G):
                out = jnp.where(lane_head == h, mixed[h * L : (h + 1) * L], out)
            cols = pl.ds(pl.multiple_of(m * Wl + g * Wg, Wg), Wg)
            hg[i * L : (i + 1) * L, cols] = out.astype(jnp.bfloat16)

    for i in range(S):
        acc[...] = jnp.zeros_like(acc)
        sq[...] = jnp.zeros_like(sq)

        def qkv_step(p, carry):
            j = nth(p)
            receive(i, j)
            if i == 0:
                wq_copy(j).wait()
            block = xg[j, i * L : (i + 1) * L, :].astype(jnp.float32)
            squares = block * block
            part = squares[:, 0:128]
            for k in range(1, Dl // 128):
                part = part + squares[:, k * 128 : (k + 1) * 128]
            sq[...] += part
            rows = pl.ds(pl.multiple_of(j * Dl, Dl), Dl)
            gained = (block * gain_ref[:, rows].astype(jnp.float32)).astype(jnp.bfloat16)
            for t in range(3):
                cols = pl.ds(t * Wl, Wl)
                acc[:, cols] += jnp.dot(gained, wq[t, rows, :], preferred_element_type=jnp.float32)
            return carry

        lax.fori_loop(0, M, qkv_step, 0)
        row_scale = lax.rsqrt(jnp.sum(sq[...], axis=1, keepdims=True) / D + NORM_EPSILON)
        qkv[...] = (acc[...] * row_scale).astype(jnp.bfloat16)
        attend(i)
        mix_act(i, start)

    wo_copy().wait()

    def hop_out(i, act):
        for c, (at, rows) in enumerate(plans[i][0]):
            act(to(ho.at[pl.ds(i * L + at, rows), :], hop_block(i, c, m),
                   hop_send.at[i, c], hop_recv.at[i, c, m], s + 1, m))

    def late_out(i, j, src, act):
        along(j, src, spread_block(i, j), spread_send.at[i], spread_recv.at[i, j], act)
        act(to(src, late_block(i, j), spread_up.at[i, j], late_recv.at[i, j], s + 1, m))

    def own_late(i):
        at, rows = plans[i][1]
        return ho.at[pl.ds(i * L + at, rows), :]

    def home(i, act):
        act(to(ho.at[pl.ds(i * L, L), :], fin, fin_send.at[i], fin_recv, i, m))

    for i in range(S):
        for k in range(1, M):
            j = lax.rem(m + k, M)
            got(hg.at[pl.ds(i * L, L), pl.ds(pl.multiple_of(j * Wl, Wl), Wl)], mix_recv.at[i, j])
        rows = slice(i * L, (i + 1) * L)
        update = jnp.dot(hg[rows, :], wo[...], preferred_element_type=jnp.float32)
        ho[rows, :] = (xg[m, rows, :].astype(jnp.float32) + update).astype(jnp.bfloat16)

        @pl.when(s < S - 1)
        def _():
            hop_out(i, start)
            if plans[i][1][1]:
                late_out(i, m, own_late(i), start)

                def late_step(p, carry):
                    j = nth(p)
                    got(spread_block(i, j), spread_recv.at[i, j])
                    late_out(i, j, spread_block(i, j), start)
                    return carry

                lax.fori_loop(1, M, late_step, 0)

        if i < S - 1:
            @pl.when(s == S - 1)
            def _():
                home(i, start)

    first_act(sent)
    for i in range(S):
        mix_act(i, sent)

        @pl.when(s > 0)
        def _():
            for c in range(len(plans[i][0])):
                hop_act(i, c, m, sent)

        @pl.when(s < S - 1)
        def _():
            hop_out(i, sent)
            if plans[i][1][1]:
                late_out(i, m, own_late(i), sent)

        if i < S - 1:
            @pl.when(s == S - 1)
            def _():
                home(i, sent)

    def drain_step(p, carry):
        j = nth(p)
        pre_act(j, sent)
        for i in range(S):
            @pl.when(s > 0)
            def _():
                for c in range(len(plans[i][0])):
                    hop_act(i, c, j, sent)

            if plans[i][1][1]:
                @pl.when(s < S - 1)
                def _():
                    late_out(i, j, spread_block(i, j), sent)

        return carry

    lax.fori_loop(1, M, drain_step, 0)

    @pl.when(s == S - 1)
    def _():
        o_ref[...] = ho[(S - 1) * L :, :]

    @pl.when(s < S - 1)
    def _():
        got(fin, fin_recv)
        o_ref[...] = fin[...]


def solution(mesh):
    S, M = mesh.shape["section"], mesh.shape["mp"]

    def shards(micro_inputs, qkv_weight, out_weight, norm_gain, position_bias):
        L, Dl = micro_inputs.shape[1:]
        D = qkv_weight.shape[1]
        Wl = qkv_weight.shape[3]
        H = position_bias.shape[0]
        R = S * L
        G = head_group(H, Wl // H)
        plans = [relay_chunks(i, S, L) for i in range(S)]
        parts = max(len(hops) for hops, _ in plans)
        late_rows = max(rows for _, (_, rows) in plans)
        buckets = jnp.asarray(bucket_table(L, position_bias.shape[1], REACH).T)
        wq = jnp.transpose(qkv_weight[0], (1, 0, 2))
        bf16, f32 = jnp.bfloat16, jnp.float32
        dma = pltpu.SemaphoreType.DMA
        vmem = pl.BlockSpec(memory_space=pltpu.VMEM)
        out = pl.pallas_call(
            functools.partial(kernel, (S, M, L, H, Wl // H)),
            out_shape=jax.ShapeDtypeStruct((L, Dl), bf16),
            in_specs=[
                vmem, vmem, vmem, pl.BlockSpec(memory_space=pltpu.SMEM),
                pl.BlockSpec(memory_space=pl.ANY), pl.BlockSpec(memory_space=pl.ANY),
            ],
            out_specs=vmem,
            scratch_shapes=[
                pltpu.VMEM((M, L, Dl), bf16),
                pltpu.VMEM((M, R, Dl), bf16),
                pltpu.VMEM((R, M * Wl), bf16),
                pltpu.VMEM((S, M, late_rows, Dl), bf16),
                pltpu.VMEM((R, Dl), bf16),
                pltpu.VMEM((L, Dl), bf16),
                pltpu.VMEM((3, D, Wl), bf16),
                pltpu.VMEM((M * Wl, Dl), bf16),
                pltpu.VMEM((L, 3 * Wl), f32),
                pltpu.VMEM((L, 128), f32),
                pltpu.VMEM((L, 3 * Wl), bf16),
                pltpu.VMEM((H // G, L, G * L), f32),
                pltpu.VMEM((G * L, Wl // H * G), bf16),
                dma((M,)), dma,
                dma((M,)), dma((2, M)), dma((M,)), dma((S, M)),
                dma((S, parts)), dma((S, parts, M)), dma((S, parts, 2, M)),
                dma((S, M)), dma((S, 2, M)), dma((S, M)), dma((S, M)),
                dma((S, M)), dma((S, M)),
                dma((S,)), dma,
            ],
            compiler_params=pltpu.CompilerParams(
                collective_id=0, has_side_effects=True, vmem_limit_bytes=60 * 1024 * 1024
            ),
        )(micro_inputs[0], norm_gain, buckets, position_bias, wq, out_weight[0])
        return out[None]

    in_specs = (
        P(("dp", "section"), None, "mp"),
        P("section", None, None, "mp"),
        P("section", None, "mp"),
        P("section", None),
        P("mp", None),
    )
    out_specs = P(("dp", "section"), None, "mp")
    return jax.shard_map(shards, mesh=mesh, in_specs=in_specs, out_specs=out_specs, check_vma=False)
```

```python
import functools
import math

import jax
import jax.numpy as jnp
import numpy as np
from jax import lax
from jax.experimental import pallas as pl
from jax.experimental.pallas import tpu as pltpu
from jax.sharding import PartitionSpec as P

REACH = 128
NORM_EPSILON = 0.1
MESH = pl.DeviceIdType.MESH


def bucket_table(length, bucket_count, reach_limit):
    offset = np.arange(length)[None, :] - np.arange(length)[:, None]
    half_count = bucket_count // 2
    upper_side = (offset > 0).astype(np.int32) * half_count
    distance = np.abs(offset)
    exact_count = half_count // 2
    scaled = (
        np.log(np.maximum(distance, 1) / exact_count)
        / np.log(reach_limit / exact_count)
        * (half_count - exact_count)
    )
    far_bucket = np.minimum(exact_count + scaled.astype(np.int32), half_count - 1)
    return (upper_side + np.where(distance < exact_count, distance, far_bucket)).astype(np.int32)


def relay_chunks(micro, micros, length):
    half = length // 2
    if micro == micros - 1:
        return [], (0, half), (half, length - half)
    return [(0, half), (half, length - half)], (0, 0), (0, 0)


def head_group(heads, head_size):
    return max(g for g in range(1, heads + 1) if heads % g == 0 and g * head_size <= 256)


def kernel(
    sizes,
    x_ref, gain_ref, bucket_ref, pbias_ref, wq_hbm, wo_hbm,
    o_ref,
    pre, xg, hg, spread, ho, fin, wq, wo, acc, sq, qkv, bias, head_mask,
    wq_sem, wo_sem,
    pre_recv, pre_send, pre_up, in_recv,
    hop_send, hop_recv, hop_line,
    spread_recv, spread_send, spread_up, late_recv, straight_send, straight_recv,
    mix_recv, mix_send,
    fin_send, fin_recv,
):
    S, M, L, H, hs = sizes
    Dl = x_ref.shape[1]
    Wl = H * hs
    G = head_group(H, hs)
    Wg = G * hs
    D = M * Dl
    s = lax.axis_index("section")
    m = lax.axis_index("mp")
    plans = [relay_chunks(i, S, L) for i in range(S)]

    def to(src, dst, send, recv, sec, col):
        return pltpu.make_async_remote_copy(
            src_ref=src, dst_ref=dst, send_sem=send, recv_sem=recv,
            device_id={"section": sec, "mp": col}, device_id_type=MESH,
        )

    def along(j, src, dst, send, recv, act):
        even = lax.rem(m - j + 2 * M, 2) == 0
        for reach in (2, 1):
            @pl.when((j <= m) & even & (m < M - reach))
            def _():
                act(to(src, dst, send.at[reach - 1, j], recv, s, m + reach))

            @pl.when((j >= m) & even & (m >= reach))
            def _():
                act(to(src, dst, send.at[reach + 1, j], recv, s, m - reach))

    def start(c):
        c.start()

    def sent(c):
        c.wait_send()

    def got(dst, recv):
        to(dst, dst, fin_send.at[0], recv, s, lax.rem(m + 1, M)).wait_recv()

    near = jnp.minimum(m, M - 1 - m)
    longer = jnp.where(m > M - 1 - m, -1, 1)

    def nth(p):
        k = (p + 1) // 2
        both = jnp.where(p % 2 == 1, -k, k)
        return m + jnp.where(p <= 2 * near, both, longer * (p - near))

    def wq_copy(j):
        rows = pl.ds(pl.multiple_of(j * Dl, Dl), Dl)
        return pltpu.make_async_copy(wq_hbm.at[:, rows, :], wq.at[:, rows, :], wq_sem.at[j])

    def wo_copy():
        return pltpu.make_async_copy(wo_hbm, wo, wo_sem)

    barrier = pltpu.get_barrier_semaphore()
    for o in range(S):
        for k in range(M):
            if o or k:
                pl.semaphore_signal(
                    barrier, inc=1,
                    device_id={"section": lax.rem(s + o, S), "mp": lax.rem(m + k, M)},
                    device_id_type=MESH,
                )

    for p in range(M):
        wq_copy(nth(p)).start()
    wo_copy().start()
    pl.semaphore_wait(barrier, S * M - 1)

    half = L // 2
    halves = [pl.ds(0, half), pl.ds(half, L - half)]

    def up_rows(j, c):
        return xg.at[j, pl.ds(pl.multiple_of(s * L + c * half, half), halves[c].size), :]

    def pre_part(j, c, src, act):
        along(j, src, pre.at[j, halves[c], :], pre_send.at[c], pre_recv.at[c, j], act)

        @pl.when(s > 0)
        def _():
            act(to(src, up_rows(j, c), pre_up.at[c, j], in_recv.at[s, c, j], 0, m))

    def first_act(act):
        for c in range(2):
            pre_part(m, c, x_ref.at[halves[c], :], act)

    def pre_act(j, act):
        for c in range(2):
            pre_part(j, c, pre.at[j, halves[c], :], act)

    def pre_step_on(j):
        for c in range(2):
            got(pre.at[j, halves[c], :], pre_recv.at[c, j])
            pre_part(j, c, pre.at[j, halves[c], :], start)

    first_act(start)

    for g in range(H // G):
        heads = []
        for h in range(g * G, (g + 1) * G):
            total = jnp.zeros(bucket_ref.shape, jnp.float32)
            for b in range(pbias_ref.shape[1]):
                total = jnp.where(bucket_ref[...] == b, pbias_ref[h, b], total)
            heads.append(total)
        bias[g] = jnp.concatenate(heads, axis=1)
    head_mask[...] = jnp.where(
        lax.broadcasted_iota(jnp.int32, (G * L, Wg), 0) // L
        == lax.broadcasted_iota(jnp.int32, (G * L, Wg), 1) // hs,
        1.0,
        0.0,
    ).astype(jnp.bfloat16)

    @pl.when(s > 0)
    def _():
        def pre_step(p, carry):
            j = nth(p)
            pre_step_on(j)
            return carry

        lax.fori_loop(1, M, pre_step, 0)

    def hop_block(i, c, j):
        at, rows = plans[i][0][c]
        return xg.at[j, pl.ds(i * L + at, rows), :]

    def hop_act(i, c, j, act):
        block = hop_block(i, c, j)
        along(j, block, block, hop_line.at[i, c], hop_recv.at[i, c, j], act)

    def late_block(i, j):
        at, rows = plans[i][1]
        return xg.at[j, pl.ds(i * L + at, rows), :]

    def straight_block(i, j):
        at, rows = plans[i][2]
        return xg.at[j, pl.ds(i * L + at, rows), :]

    def spread_block(i, j):
        return spread.at[i, j, pl.ds(0, plans[i][1][1]), :]

    def receive(i, j):
        @pl.when(s == 0)
        def _():
            if i:
                for c in range(2):
                    got(xg.at[j, pl.ds(i * L + c * half, halves[c].size), :], in_recv.at[i, c, j])
            else:
                @pl.when(j == m)
                def _():
                    xg[m, 0:L, :] = x_ref[...]

                @pl.when(j != m)
                def _():
                    pre_step_on(j)
                    xg[j, 0:L, :] = pre[j]

        @pl.when(s > 0)
        def _():
            for c in range(len(plans[i][0])):
                got(hop_block(i, c, j), hop_recv.at[i, c, j])
                hop_act(i, c, j, start)
            if plans[i][1][1]:
                got(late_block(i, j), late_recv.at[i, j])
            if plans[i][2][1]:
                got(straight_block(i, j), straight_recv.at[i, j])

    def mix_act(i, act):
        block = hg.at[pl.ds(i * L, L), pl.ds(pl.multiple_of(m * Wl, Wl), Wl)]
        for k in range(1, M):
            col = lax.rem(m + k, M)
            act(to(block, block, mix_send.at[i, k], mix_recv.at[i, m], s, col))

    scale = 1.0 / math.sqrt(hs)
    lane_head = lax.broadcasted_iota(jnp.int32, (L, Wg), 1) // hs

    def attend(i):
        for g in range(H // G):
            q = qkv[:, g * Wg : (g + 1) * Wg]
            k = qkv[:, Wl + g * Wg : Wl + (g + 1) * Wg]
            v = qkv[:, 2 * Wl + g * Wg : 2 * Wl + (g + 1) * Wg]
            apart = jnp.concatenate([q] * G, axis=0) * head_mask[...]
            scores = lax.dot_general(
                k, apart, (((1,), (1,)), ((), ())), preferred_element_type=jnp.float32
            ) * scale + bias[g]
            weights = jnp.exp(scores - jnp.max(scores, axis=0, keepdims=True))
            probs = (weights / jnp.sum(weights, axis=0, keepdims=True)).astype(jnp.bfloat16)
            mixed = lax.dot_general(
                probs, v, (((0,), (0,)), ((), ())), preferred_element_type=jnp.float32
            )
            out = mixed[0:L]
            for h in range(1, G):
                out = jnp.where(lane_head == h, mixed[h * L : (h + 1) * L], out)
            cols = pl.ds(pl.multiple_of(m * Wl + g * Wg, Wg), Wg)
            hg[i * L : (i + 1) * L, cols] = out.astype(jnp.bfloat16)

    for i in range(S):
        acc[...] = jnp.zeros_like(acc)
        sq[...] = jnp.zeros_like(sq)

        def qkv_step(p, carry):
            j = nth(p)
            receive(i, j)
            if i == 0:
                wq_copy(j).wait()
            block = xg[j, i * L : (i + 1) * L, :].astype(jnp.float32)
            squares = block * block
            part = squares[:, 0:128]
            for k in range(1, Dl // 128):
                part = part + squares[:, k * 128 : (k + 1) * 128]
            sq[...] += part
            rows = pl.ds(pl.multiple_of(j * Dl, Dl), Dl)
            gained = (block * gain_ref[:, rows].astype(jnp.float32)).astype(jnp.bfloat16)
            for t in range(3):
                cols = pl.ds(t * Wl, Wl)
                acc[:, cols] += jnp.dot(gained, wq[t, rows, :], preferred_element_type=jnp.float32)
            return carry

        lax.fori_loop(0, M, qkv_step, 0)
        row_scale = lax.rsqrt(jnp.sum(sq[...], axis=1, keepdims=True) / D + NORM_EPSILON)
        qkv[...] = (acc[...] * row_scale).astype(jnp.bfloat16)
        attend(i)
        mix_act(i, start)

    wo_copy().wait()

    def hop_out(i, act):
        for c, (at, rows) in enumerate(plans[i][0]):
            act(to(ho.at[pl.ds(i * L + at, rows), :], hop_block(i, c, m),
                   hop_send.at[i, c], hop_recv.at[i, c, m], s + 1, m))

    def late_out(i, j, src, act):
        along(j, src, spread_block(i, j), spread_send.at[i], spread_recv.at[i, j], act)
        act(to(src, late_block(i, j), spread_up.at[i, j], late_recv.at[i, j], s + 1, m))

    def straight_out(i, act):
        at, rows = plans[i][2]
        for k in range(M):
            act(to(ho.at[pl.ds(i * L + at, rows), :], straight_block(i, m),
                   straight_send.at[i, k], straight_recv.at[i, m], s + 1, lax.rem(m + k, M)))

    def own_late(i):
        at, rows = plans[i][1]
        return ho.at[pl.ds(i * L + at, rows), :]

    def home(i, act):
        act(to(ho.at[pl.ds(i * L, L), :], fin, fin_send.at[i], fin_recv, i, m))

    for i in range(S):
        for k in range(1, M):
            j = lax.rem(m + k, M)
            got(hg.at[pl.ds(i * L, L), pl.ds(pl.multiple_of(j * Wl, Wl), Wl)], mix_recv.at[i, j])
        rows = slice(i * L, (i + 1) * L)
        update = jnp.dot(hg[rows, :], wo[...], preferred_element_type=jnp.float32)
        ho[rows, :] = (xg[m, rows, :].astype(jnp.float32) + update).astype(jnp.bfloat16)

        @pl.when(s < S - 1)
        def _():
            hop_out(i, start)
            if plans[i][1][1]:
                late_out(i, m, own_late(i), start)
            if plans[i][2][1]:
                straight_out(i, start)
            if plans[i][1][1]:

                def late_step(p, carry):
                    j = nth(p)
                    got(spread_block(i, j), spread_recv.at[i, j])
                    late_out(i, j, spread_block(i, j), start)
                    return carry

                lax.fori_loop(1, M, late_step, 0)

        if i < S - 1:
            @pl.when(s == S - 1)
            def _():
                home(i, start)

    first_act(sent)
    for i in range(S):
        mix_act(i, sent)

        @pl.when(s > 0)
        def _():
            for c in range(len(plans[i][0])):
                hop_act(i, c, m, sent)

        @pl.when(s < S - 1)
        def _():
            hop_out(i, sent)
            if plans[i][1][1]:
                late_out(i, m, own_late(i), sent)
            if plans[i][2][1]:
                straight_out(i, sent)

        if i < S - 1:
            @pl.when(s == S - 1)
            def _():
                home(i, sent)

    def drain_step(p, carry):
        j = nth(p)
        pre_act(j, sent)
        for i in range(S):
            @pl.when(s > 0)
            def _():
                for c in range(len(plans[i][0])):
                    hop_act(i, c, j, sent)

            if plans[i][1][1]:
                @pl.when(s < S - 1)
                def _():
                    late_out(i, j, spread_block(i, j), sent)

        return carry

    lax.fori_loop(1, M, drain_step, 0)

    @pl.when(s == S - 1)
    def _():
        o_ref[...] = ho[(S - 1) * L :, :]

    @pl.when(s < S - 1)
    def _():
        got(fin, fin_recv)
        o_ref[...] = fin[...]


def solution(mesh):
    S, M = mesh.shape["section"], mesh.shape["mp"]

    def shards(micro_inputs, qkv_weight, out_weight, norm_gain, position_bias):
        L, Dl = micro_inputs.shape[1:]
        D = qkv_weight.shape[1]
        Wl = qkv_weight.shape[3]
        H = position_bias.shape[0]
        R = S * L
        G = head_group(H, Wl // H)
        plans = [relay_chunks(i, S, L) for i in range(S)]
        parts = max(1, *(len(hops) for hops, _, _ in plans))
        late_rows = max(rows for _, (_, rows), _ in plans)
        buckets = jnp.asarray(bucket_table(L, position_bias.shape[1], REACH).T)
        wq = jnp.transpose(qkv_weight[0], (1, 0, 2))
        bf16, f32 = jnp.bfloat16, jnp.float32
        dma = pltpu.SemaphoreType.DMA
        vmem = pl.BlockSpec(memory_space=pltpu.VMEM)
        out = pl.pallas_call(
            functools.partial(kernel, (S, M, L, H, Wl // H)),
            out_shape=jax.ShapeDtypeStruct((L, Dl), bf16),
            in_specs=[
                vmem, vmem, vmem, pl.BlockSpec(memory_space=pltpu.SMEM),
                pl.BlockSpec(memory_space=pltpu.HBM), pl.BlockSpec(memory_space=pltpu.HBM),
            ],
            out_specs=vmem,
            scratch_shapes=[
                pltpu.VMEM((M, L, Dl), bf16),
                pltpu.VMEM((M, R, Dl), bf16),
                pltpu.VMEM((R, M * Wl), bf16),
                pltpu.VMEM((S, M, late_rows, Dl), bf16),
                pltpu.VMEM((R, Dl), bf16),
                pltpu.VMEM((L, Dl), bf16),
                pltpu.VMEM((3, D, Wl), bf16),
                pltpu.VMEM((M * Wl, Dl), bf16),
                pltpu.VMEM((L, 3 * Wl), f32),
                pltpu.VMEM((L, 128), f32),
                pltpu.VMEM((L, 3 * Wl), bf16),
                pltpu.VMEM((H // G, L, G * L), f32),
                pltpu.VMEM((G * L, Wl // H * G), bf16),
                dma((M,)), dma,
                dma((2, M)), dma((2, 4, M)), dma((2, M)), dma((S, 2, M)),
                dma((S, parts)), dma((S, parts, M)), dma((S, parts, 4, M)),
                dma((S, M)), dma((S, 4, M)), dma((S, M)), dma((S, M)), dma((S, M)), dma((S, M)),
                dma((S, M)), dma((S, M)),
                dma((S,)), dma,
            ],
            compiler_params=pltpu.CompilerParams(
                collective_id=0, has_side_effects=True, vmem_limit_bytes=60 * 1024 * 1024
            ),
        )(micro_inputs[0], norm_gain, buckets, position_bias, wq, out_weight[0])
        return out[None]

    in_specs = (
        P(("dp", "section"), None, "mp"),
        P("section", None, None, "mp"),
        P("section", None, "mp"),
        P("section", None),
        P("mp", None),
    )
    out_specs = P(("dp", "section"), None, "mp")
    return jax.shard_map(shards, mesh=mesh, in_specs=in_specs, out_specs=out_specs, check_vma=False)
```

```python
import functools
import math

import jax
import jax.numpy as jnp
import numpy as np
from jax import lax
from jax.experimental import pallas as pl
from jax.experimental.pallas import tpu as pltpu
from jax.sharding import PartitionSpec as P

REACH = 128
NORM_EPSILON = 0.1
MESH = pl.DeviceIdType.MESH


def bucket_table(length, bucket_count, reach_limit):
    offset = np.arange(length)[None, :] - np.arange(length)[:, None]
    half_count = bucket_count // 2
    upper_side = (offset > 0).astype(np.int32) * half_count
    distance = np.abs(offset)
    exact_count = half_count // 2
    scaled = (
        np.log(np.maximum(distance, 1) / exact_count)
        / np.log(reach_limit / exact_count)
        * (half_count - exact_count)
    )
    far_bucket = np.minimum(exact_count + scaled.astype(np.int32), half_count - 1)
    return (upper_side + np.where(distance < exact_count, distance, far_bucket)).astype(np.int32)


def relay_chunks(micro, micros, length):
    half = length // 2
    if micro == micros - 1:
        return [], (0, half), (half, length - half)
    return [(0, half), (half, length - half)], (0, 0), (0, 0)


def head_group(heads, head_size):
    return max(g for g in range(1, heads + 1) if heads % g == 0 and g * head_size <= 256)


def kernel(
    sizes,
    x_ref, gain_ref, bucket_ref, pbias_ref, wq_hbm, wo_hbm,
    o_ref,
    pre, xg, hg, spread, ho, fin, wq, wo, acc, sq, qkv, bias, head_mask,
    wq_sem, wo_sem,
    pre_recv, pre_send, pre_up, in_recv,
    hop_send, hop_recv, hop_line,
    spread_recv, spread_send, spread_up, late_recv, straight_send, straight_recv,
    mix_recv, mix_send,
    fin_send, fin_recv,
):
    S, M, L, H, hs = sizes
    Dl = x_ref.shape[1]
    Wl = H * hs
    G = head_group(H, hs)
    Wg = G * hs
    D = M * Dl
    s = lax.axis_index("section")
    m = lax.axis_index("mp")
    plans = [relay_chunks(i, S, L) for i in range(S)]

    def to(src, dst, send, recv, sec, col):
        return pltpu.make_async_remote_copy(
            src_ref=src, dst_ref=dst, send_sem=send, recv_sem=recv,
            device_id={"section": sec, "mp": col}, device_id_type=MESH,
        )

    def along(j, src, dst, send, recv, act):
        even = lax.rem(m - j + 2 * M, 2) == 0
        for reach in (2, 1):
            @pl.when((j <= m) & even & (m < M - reach))
            def _():
                act(to(src, dst, send.at[reach - 1, j], recv, s, m + reach))

            @pl.when((j >= m) & even & (m >= reach))
            def _():
                act(to(src, dst, send.at[reach + 1, j], recv, s, m - reach))

    def start(c):
        c.start()

    def sent(c):
        c.wait_send()

    def got(dst, recv):
        to(dst, dst, fin_send.at[0], recv, s, lax.rem(m + 1, M)).wait_recv()

    near = jnp.minimum(m, M - 1 - m)
    longer = jnp.where(m > M - 1 - m, -1, 1)

    def nth(p):
        k = (p + 1) // 2
        both = jnp.where(p % 2 == 1, -k, k)
        return m + jnp.where(p <= 2 * near, both, longer * (p - near))

    def wq_copy(j):
        rows = pl.ds(pl.multiple_of(j * Dl, Dl), Dl)
        return pltpu.make_async_copy(wq_hbm.at[:, rows, :], wq.at[:, rows, :], wq_sem.at[j])

    def wo_copy():
        return pltpu.make_async_copy(wo_hbm, wo, wo_sem)

    barrier = pltpu.get_barrier_semaphore()
    for o in range(S):
        for k in range(M):
            if o or k:
                pl.semaphore_signal(
                    barrier, inc=1,
                    device_id={"section": lax.rem(s + o, S), "mp": lax.rem(m + k, M)},
                    device_id_type=MESH,
                )

    for p in range(M):
        wq_copy(nth(p)).start()
    wo_copy().start()
    pl.semaphore_wait(barrier, S * M - 1)

    half = L // 2
    halves = [pl.ds(0, half), pl.ds(half, L - half)]

    def up_rows(j, c):
        return xg.at[j, pl.ds(pl.multiple_of(s * L + c * half, half), halves[c].size), :]

    def pre_part(j, c, src, act):
        along(j, src, pre.at[j, halves[c], :], pre_send.at[c], pre_recv.at[c, j], act)

        @pl.when(s > 0)
        def _():
            act(to(src, up_rows(j, c), pre_up.at[c, j], in_recv.at[s, c, j], 0, m))

    def first_act(act):
        for c in range(2):
            pre_part(m, c, x_ref.at[halves[c], :], act)

    def pre_act(j, act):
        for c in range(2):
            pre_part(j, c, pre.at[j, halves[c], :], act)

    def pre_step_on(j):
        for c in range(2):
            got(pre.at[j, halves[c], :], pre_recv.at[c, j])
            pre_part(j, c, pre.at[j, halves[c], :], start)

    first_act(start)

    for g in range(H // G):
        heads = []
        for h in range(g * G, (g + 1) * G):
            total = jnp.zeros(bucket_ref.shape, jnp.float32)
            for b in range(pbias_ref.shape[1]):
                total = jnp.where(bucket_ref[...] == b, pbias_ref[h, b], total)
            heads.append(total)
        bias[g] = jnp.concatenate(heads, axis=1)
    head_mask[...] = jnp.where(
        lax.broadcasted_iota(jnp.int32, (G * L, Wg), 0) // L
        == lax.broadcasted_iota(jnp.int32, (G * L, Wg), 1) // hs,
        1.0,
        0.0,
    ).astype(jnp.bfloat16)

    @pl.when(s > 0)
    def _():
        def pre_step(p, carry):
            j = nth(p)
            pre_step_on(j)
            return carry

        lax.fori_loop(1, M, pre_step, 0)

    def hop_block(i, c, j):
        at, rows = plans[i][0][c]
        return xg.at[j, pl.ds(i * L + at, rows), :]

    def hop_act(i, c, j, act):
        block = hop_block(i, c, j)
        along(j, block, block, hop_line.at[i, c], hop_recv.at[i, c, j], act)

    def late_block(i, j):
        at, rows = plans[i][1]
        return xg.at[j, pl.ds(i * L + at, rows), :]

    def straight_block(i, j):
        at, rows = plans[i][2]
        return xg.at[j, pl.ds(i * L + at, rows), :]

    def spread_block(i, j):
        return spread.at[i, j, pl.ds(0, plans[i][1][1]), :]

    def receive(i, j):
        @pl.when(s == 0)
        def _():
            if i:
                for c in range(2):
                    got(xg.at[j, pl.ds(i * L + c * half, halves[c].size), :], in_recv.at[i, c, j])
            else:
                @pl.when(j == m)
                def _():
                    xg[m, 0:L, :] = x_ref[...]

                @pl.when(j != m)
                def _():
                    pre_step_on(j)
                    xg[j, 0:L, :] = pre[j]

        @pl.when(s > 0)
        def _():
            for c in range(len(plans[i][0])):
                got(hop_block(i, c, j), hop_recv.at[i, c, j])
                hop_act(i, c, j, start)
            if plans[i][1][1]:
                got(late_block(i, j), late_recv.at[i, j])
            if plans[i][2][1]:
                got(straight_block(i, j), straight_recv.at[i, j])

    def mix_act(i, act):
        block = hg.at[pl.ds(i * L, L), pl.ds(pl.multiple_of(m * Wl, Wl), Wl)]
        for p in reversed(range(1, M)):
            act(to(block, block, mix_send.at[i, p], mix_recv.at[i, m], s, nth(p)))

    scale = 1.0 / math.sqrt(hs)
    lane_head = lax.broadcasted_iota(jnp.int32, (L, Wg), 1) // hs

    def attend(i):
        for g in range(H // G):
            q = qkv[:, g * Wg : (g + 1) * Wg]
            k = qkv[:, Wl + g * Wg : Wl + (g + 1) * Wg]
            v = qkv[:, 2 * Wl + g * Wg : 2 * Wl + (g + 1) * Wg]
            apart = jnp.concatenate([q] * G, axis=0) * head_mask[...]
            scores = lax.dot_general(
                k, apart, (((1,), (1,)), ((), ())), preferred_element_type=jnp.float32
            ) * scale + bias[g]
            weights = jnp.exp(scores - jnp.max(scores, axis=0, keepdims=True))
            probs = (weights / jnp.sum(weights, axis=0, keepdims=True)).astype(jnp.bfloat16)
            mixed = lax.dot_general(
                probs, v, (((0,), (0,)), ((), ())), preferred_element_type=jnp.float32
            )
            out = mixed[0:L]
            for h in range(1, G):
                out = jnp.where(lane_head == h, mixed[h * L : (h + 1) * L], out)
            cols = pl.ds(pl.multiple_of(m * Wl + g * Wg, Wg), Wg)
            hg[i * L : (i + 1) * L, cols] = out.astype(jnp.bfloat16)

    for i in range(S):
        acc[...] = jnp.zeros_like(acc)
        sq[...] = jnp.zeros_like(sq)

        def qkv_step(p, carry):
            j = nth(p)
            receive(i, j)
            if i == 0:
                wq_copy(j).wait()
            block = xg[j, i * L : (i + 1) * L, :].astype(jnp.float32)
            squares = block * block
            part = squares[:, 0:128]
            for k in range(1, Dl // 128):
                part = part + squares[:, k * 128 : (k + 1) * 128]
            sq[...] += part
            rows = pl.ds(pl.multiple_of(j * Dl, Dl), Dl)
            gained = (block * gain_ref[:, rows].astype(jnp.float32)).astype(jnp.bfloat16)
            for t in range(3):
                cols = pl.ds(t * Wl, Wl)
                acc[:, cols] += jnp.dot(gained, wq[t, rows, :], preferred_element_type=jnp.float32)
            return carry

        lax.fori_loop(0, M, qkv_step, 0)
        row_scale = lax.rsqrt(jnp.sum(sq[...], axis=1, keepdims=True) / D + NORM_EPSILON)
        qkv[...] = (acc[...] * row_scale).astype(jnp.bfloat16)
        attend(i)
        mix_act(i, start)

    wo_copy().wait()

    def hop_out(i, act):
        for c, (at, rows) in enumerate(plans[i][0]):
            act(to(ho.at[pl.ds(i * L + at, rows), :], hop_block(i, c, m),
                   hop_send.at[i, c], hop_recv.at[i, c, m], s + 1, m))

    def late_out(i, j, src, act):
        along(j, src, spread_block(i, j), spread_send.at[i], spread_recv.at[i, j], act)
        act(to(src, late_block(i, j), spread_up.at[i, j], late_recv.at[i, j], s + 1, m))

    def straight_out(i, act):
        at, rows = plans[i][2]
        for p in reversed(range(M)):
            act(to(ho.at[pl.ds(i * L + at, rows), :], straight_block(i, m),
                   straight_send.at[i, p], straight_recv.at[i, m], s + 1, nth(p)))

    def own_late(i):
        at, rows = plans[i][1]
        return ho.at[pl.ds(i * L + at, rows), :]

    def home(i, act):
        act(to(ho.at[pl.ds(i * L, L), :], fin, fin_send.at[i], fin_recv, i, m))

    for i in range(S):
        for k in range(1, M):
            j = lax.rem(m + k, M)
            got(hg.at[pl.ds(i * L, L), pl.ds(pl.multiple_of(j * Wl, Wl), Wl)], mix_recv.at[i, j])
        rows = slice(i * L, (i + 1) * L)
        update = jnp.dot(hg[rows, :], wo[...], preferred_element_type=jnp.float32)
        ho[rows, :] = (xg[m, rows, :].astype(jnp.float32) + update).astype(jnp.bfloat16)

        @pl.when(s < S - 1)
        def _():
            hop_out(i, start)
            if plans[i][1][1]:
                late_out(i, m, own_late(i), start)
            if plans[i][2][1]:
                straight_out(i, start)
            if plans[i][1][1]:

                def late_step(p, carry):
                    j = nth(p)
                    got(spread_block(i, j), spread_recv.at[i, j])
                    late_out(i, j, spread_block(i, j), start)
                    return carry

                lax.fori_loop(1, M, late_step, 0)

        if i < S - 1:
            @pl.when(s == S - 1)
            def _():
                home(i, start)

    first_act(sent)
    for i in range(S):
        mix_act(i, sent)

        @pl.when(s > 0)
        def _():
            for c in range(len(plans[i][0])):
                hop_act(i, c, m, sent)

        @pl.when(s < S - 1)
        def _():
            hop_out(i, sent)
            if plans[i][1][1]:
                late_out(i, m, own_late(i), sent)
            if plans[i][2][1]:
                straight_out(i, sent)

        if i < S - 1:
            @pl.when(s == S - 1)
            def _():
                home(i, sent)

    def drain_step(p, carry):
        j = nth(p)
        pre_act(j, sent)
        for i in range(S):
            @pl.when(s > 0)
            def _():
                for c in range(len(plans[i][0])):
                    hop_act(i, c, j, sent)

            if plans[i][1][1]:
                @pl.when(s < S - 1)
                def _():
                    late_out(i, j, spread_block(i, j), sent)

        return carry

    lax.fori_loop(1, M, drain_step, 0)

    @pl.when(s == S - 1)
    def _():
        o_ref[...] = ho[(S - 1) * L :, :]

    @pl.when(s < S - 1)
    def _():
        got(fin, fin_recv)
        o_ref[...] = fin[...]


def solution(mesh):
    S, M = mesh.shape["section"], mesh.shape["mp"]

    def shards(micro_inputs, qkv_weight, out_weight, norm_gain, position_bias):
        L, Dl = micro_inputs.shape[1:]
        D = qkv_weight.shape[1]
        Wl = qkv_weight.shape[3]
        H = position_bias.shape[0]
        R = S * L
        G = head_group(H, Wl // H)
        plans = [relay_chunks(i, S, L) for i in range(S)]
        parts = max(1, *(len(hops) for hops, _, _ in plans))
        late_rows = max(rows for _, (_, rows), _ in plans)
        buckets = jnp.asarray(bucket_table(L, position_bias.shape[1], REACH).T)
        wq = jnp.transpose(qkv_weight[0], (1, 0, 2))
        bf16, f32 = jnp.bfloat16, jnp.float32
        dma = pltpu.SemaphoreType.DMA
        vmem = pl.BlockSpec(memory_space=pltpu.VMEM)
        out = pl.pallas_call(
            functools.partial(kernel, (S, M, L, H, Wl // H)),
            out_shape=jax.ShapeDtypeStruct((L, Dl), bf16),
            in_specs=[
                vmem, vmem, vmem, pl.BlockSpec(memory_space=pltpu.SMEM),
                pl.BlockSpec(memory_space=pltpu.HBM), pl.BlockSpec(memory_space=pltpu.HBM),
            ],
            out_specs=vmem,
            scratch_shapes=[
                pltpu.VMEM((M, L, Dl), bf16),
                pltpu.VMEM((M, R, Dl), bf16),
                pltpu.VMEM((R, M * Wl), bf16),
                pltpu.VMEM((S, M, late_rows, Dl), bf16),
                pltpu.VMEM((R, Dl), bf16),
                pltpu.VMEM((L, Dl), bf16),
                pltpu.VMEM((3, D, Wl), bf16),
                pltpu.VMEM((M * Wl, Dl), bf16),
                pltpu.VMEM((L, 3 * Wl), f32),
                pltpu.VMEM((L, 128), f32),
                pltpu.VMEM((L, 3 * Wl), bf16),
                pltpu.VMEM((H // G, L, G * L), f32),
                pltpu.VMEM((G * L, Wl // H * G), bf16),
                dma((M,)), dma,
                dma((2, M)), dma((2, 4, M)), dma((2, M)), dma((S, 2, M)),
                dma((S, parts)), dma((S, parts, M)), dma((S, parts, 4, M)),
                dma((S, M)), dma((S, 4, M)), dma((S, M)), dma((S, M)), dma((S, M)), dma((S, M)),
                dma((S, M)), dma((S, M)),
                dma((S,)), dma,
            ],
            compiler_params=pltpu.CompilerParams(
                collective_id=0, has_side_effects=True, vmem_limit_bytes=60 * 1024 * 1024
            ),
        )(micro_inputs[0], norm_gain, buckets, position_bias, wq, out_weight[0])
        return out[None]

    in_specs = (
        P(("dp", "section"), None, "mp"),
        P("section", None, None, "mp"),
        P("section", None, "mp"),
        P("section", None),
        P("mp", None),
    )
    out_specs = P(("dp", "section"), None, "mp")
    return jax.shard_map(shards, mesh=mesh, in_specs=in_specs, out_specs=out_specs, check_vma=False)
```
